32 devices in a mesh: rep: 4 (over x, y), dp: 8 (over z, core).
Axes of the slice: x: 2, y: 2, z: 4, core: 2. Of those that a mesh axis runs over, the one named last changes fastest.
Arguments:
- x: bfloat16 [32, 2048, 640], P(('rep', 'dp')), parts along dimension 0
- dy: bfloat16 [32, 2048, 640], P(('rep', 'dp')), parts along dimension 0
- w_gate: bfloat16 [2, 640, 2048], replicated
- w_up: bfloat16 [2, 640, 2048], replicated
- w_down: bfloat16 [2, 2048, 640], replicated
- m_w_gate: float32 [2, 640, 2048], replicated
- m_w_up: float32 [2, 640, 2048], replicated
- m_w_down: float32 [2, 2048, 640], replicated
- v_w_gate: float32 [2, 640, 2048], replicated
- v_w_up: float32 [2, 640, 2048], replicated
- v_w_down: float32 [2, 2048, 640], replicated
Outputs:
- output 1: bfloat16 [8, 640, 2048], P('rep'), parts along dimension 0
- output 2: bfloat16 [8, 640, 2048], P('rep'), parts along dimension 0
- output 3: bfloat16 [8, 2048, 640], P('rep'), parts along dimension 0
- output 4: float32 [8, 640, 2048], P('rep'), parts along dimension 0
- output 5: float32 [8, 640, 2048], P('rep'), parts along dimension 0
- output 6: float32 [8, 2048, 640], P('rep'), parts along dimension 0
- output 7: float32 [8, 640, 2048], P('rep'), parts along dimension 0
- output 8: float32 [8, 640, 2048], P('rep'), parts along dimension 0
- output 9: float32 [8, 2048, 640], P('rep'), parts along dimension 0
There are 4 independent parts. The reference program is written for one: setup_inputs(seed, part) draws one part's arguments, and reference() takes and returns one part's arrays. A program takes and returns all parts, laid end to end along the dimension named above; an argument that names none is the same for every part.
All inputs are finite; a program needn't handle non-finite values.
Results may differ from the reference program's by a relative error of at most 0.022.
Values are sent between devices in bfloat16 or wider.
A program may use at most 2.25 GiB of HBM per device.

```python
import jax
import jax.numpy as jnp
from jax import lax

SEQUENCES = 8
TOKENS = 2048
D = 640
FF = 2048
LAYERS = 2
NAMES = ("w_gate", "w_up", "w_down")
SHAPES = {"w_gate": (LAYERS, D, FF), "w_up": (LAYERS, D, FF), "w_down": (LAYERS, FF, D)}


def bump(key, n, height):
    away = (jnp.arange(n, dtype=jnp.int32) - jax.random.randint(key, (), 0, n, jnp.int32)) % n
    return jnp.where(away < n // 8, height, 1.0)


def together(key, own, strength):
    shared = jax.random.normal(key, own.shape[1:], jnp.float32)
    return (own + strength * shared) * lax.rsqrt(1 + strength * strength)


def setup_inputs(seed: int = 0, part: int = 0) -> dict:
    kx, kdy, ka, kb, kz, kf, kh, kl, *keys = jax.random.split(jax.random.key(seed), 8 + 3 * len(NAMES))
    kx, kdy, ka, kb = (jax.random.fold_in(k, part) for k in (kx, kdy, ka, kb))
    kw, km, kv = (keys[i::3] for i in range(3))
    shape = (SEQUENCES, TOKENS, D)
    much_x, much_dy = jax.random.uniform(kz, (2,), jnp.float32, 0.0, 1.0)
    loud = 2.0 ** jax.random.uniform(jax.random.fold_in(kz, 1), (), jnp.float32, -1.0, 2.0)
    layers = 2.0 ** jax.random.uniform(kl, (LAYERS, 1, 1), jnp.float32, -1.0, 1.0)
    x = together(ka, jax.random.normal(kx, shape, jnp.float32), much_x) * bump(kf, D, 4.0)
    dy = together(kb, jax.random.normal(kdy, shape, jnp.float32), much_dy)
    drawn = {"x": x.astype(jnp.bfloat16), "dy": (loud * dy * (SEQUENCES * TOKENS) ** -0.5).astype(jnp.bfloat16)}
    for key, name in zip(kw, NAMES, strict=True):
        w = jax.random.normal(key, SHAPES[name], jnp.float32) * SHAPES[name][1] ** -0.5
        drawn[name] = (w * {"w_gate": 1.0, "w_up": bump(kh, FF, 4.0), "w_down": layers}[name]).astype(jnp.bfloat16)
    for key, name in zip(km, NAMES, strict=True):
        drawn[f"m_{name}"] = 0.1 * jax.random.normal(key, SHAPES[name], jnp.float32)
    for key, name in zip(kv, NAMES, strict=True):
        drawn[f"v_{name}"] = jax.random.uniform(key, SHAPES[name], jnp.float32, 0.005, 0.015)
    return drawn


def matmul(a, w):
    return jnp.dot(a, w, preferred_element_type=jnp.float32).astype(jnp.bfloat16)


def normed(h):
    wide = h.astype(jnp.float32)
    scale = lax.rsqrt(jnp.mean(wide**2, -1, keepdims=True) + 1e-6)
    return (wide * scale).astype(jnp.bfloat16)


def layer(h, w):
    a = normed(h)
    gate = jnp.dot(a, w["w_gate"], preferred_element_type=jnp.float32)
    up = jnp.dot(a, w["w_up"], preferred_element_type=jnp.float32)
    return h + matmul((jax.nn.silu(gate) * up).astype(jnp.bfloat16), w["w_down"])


def adamw(w, m, v, g):
    m = 0.9 * m + 0.1 * g
    v = 0.95 * v + 0.05 * g * g
    step = m * lax.rsqrt(v + 1e-8) + 0.1 * w
    return (w - 0.02 * step).astype(jnp.bfloat16), m, v


def stack(weights, h):
    return lax.scan(lambda h, w: (layer(h, w), None), h, weights)[0]


def reference(x, dy, w_gate, w_up, w_down, m_w_gate, m_w_up, m_w_down, v_w_gate, v_w_up, v_w_down):
    weights = dict(zip(NAMES, (w_gate, w_up, w_down), strict=True))

    def take(so_far, sequence):
        h, by_y = sequence
        _, back = jax.vjp(lambda w: stack(w, h), weights)
        return jax.tree.map(lambda total, term: total + term.astype(jnp.float32), so_far, back(by_y)[0]), None

    none_yet = {name: jnp.zeros(w.shape, jnp.float32) for name, w in weights.items()}
    by_weights, _ = lax.scan(take, none_yet, (x, dy))
    gradients = [by_weights[name].astype(jnp.bfloat16).astype(jnp.float32) for name in NAMES]
    new = [
        adamw(w.astype(jnp.float32), m, v, g)
        for w, m, v, g in zip((w_gate, w_up, w_down), (m_w_gate, m_w_up, m_w_down), (v_w_gate, v_w_up, v_w_down), gradients, strict=True)
    ]
    return tuple(one[which] for which in range(3) for one in new)
```

```python
import functools

import jax
import jax.numpy as jnp
from jax import lax
from jax.experimental import pallas as pl
from jax.experimental.pallas import tpu as pltpu
from jax.sharding import PartitionSpec as P

T, D, FF = 2048, 640, 2048
FS = 256
SLICES = FF // FS
CHUNKS = 2 * SLICES * 3
SLOTS = 8
LAST = 12
HALF = D // 2
ROWS = 512
F32, BF16 = jnp.float32, jnp.bfloat16
MESH = pl.DeviceIdType.MESH


def normed(h):
    wide = h.astype(F32)
    scale = lax.rsqrt(jnp.mean(wide**2, -1, keepdims=True) + 1e-6)
    return (wide * scale).astype(BF16)


def matmul(a, w):
    return jnp.dot(a, w, preferred_element_type=F32).astype(BF16)


def adamw(w, m, v, g):
    m = 0.9 * m + 0.1 * g
    v = 0.95 * v + 0.05 * g * g
    step = m * lax.rsqrt(v + 1e-8) + 0.1 * w
    return (w - 0.02 * step).astype(BF16), m, v


def dot_t(a, b):
    return lax.dot_general(a, b, (((1,), (1,)), ((), ())), preferred_element_type=F32)


def kernel(
    a0_in, a1_in, h_in, dy_in, wg_in, wu_in, wd_in, out,
    a, at, dz, dzt, h, da, wgu, wd, act, dgu,
    g, xb, ab, bb, sb, tot,
    load_sem, w_sem, sx, rx, ss, ra, rb, sc, rc, sy, ry, so,
):
    at_dp = lax.axis_index("dp")
    c = lax.rem(at_dp, 2)
    z = lax.div(at_dp, 2)
    is_end = (z == 0) | (z == 3)
    is_mid = (z == 1) | (z == 2)
    partner = z * 2 + 1 - c
    inner = jnp.where(z == 0, 1, 2) * 2 + c
    outer = jnp.where(z == 1, 0, 3) * 2 + c
    across = (3 - z) * 2 + c
    own = pl.ds(pl.multiple_of(c * HALF, HALF), HALF)
    other = pl.ds(pl.multiple_of((1 - c) * HALF, HALF), HALF)

    def load(src, dst, i):
        return pltpu.make_async_copy(src, dst, load_sem.at[i])

    loads = [
        load(a1_in, a.at[1], 0),
        load(dy_in, dz, 1),
        load(a0_in, a.at[0], 2),
        load(h_in, h, 3),
    ]

    def weights(s):
        slot = lax.rem(s, 2)
        layer = 1 - lax.div(s, SLICES)
        cols = pl.ds(pl.multiple_of(lax.rem(s, SLICES) * FS, FS), FS)
        return [
            pltpu.make_async_copy(wg_in.at[layer, :, cols], wgu.at[slot, :, pl.ds(0, FS)], w_sem.at[slot, 0]),
            pltpu.make_async_copy(wu_in.at[layer, :, cols], wgu.at[slot, :, pl.ds(FS, FS)], w_sem.at[slot, 1]),
            pltpu.make_async_copy(wd_in.at[layer, cols, :], wd.at[slot], w_sem.at[slot, 2]),
        ]

    loads[0].start()
    for copy in weights(0):
        copy.start()
    for one in loads[1:]:
        one.start()

    barrier = pltpu.get_barrier_semaphore()

    def greet(device):
        pl.semaphore_signal(barrier, inc=1, device_id={"dp": device}, device_id_type=MESH)

    greet(partner)

    @pl.when(is_end)
    def _():
        greet(inner)
        pl.semaphore_wait(barrier, 2)

    @pl.when(is_mid)
    def _():
        greet(outer)
        greet(across)
        pl.semaphore_wait(barrier, 3)

    def remote(src, dst, send, recv, device):
        return pltpu.make_async_remote_copy(
            src_ref=src, dst_ref=dst, send_sem=send, recv_sem=recv, device_id={"dp": device}, device_id_type=MESH
        )

    def copy_x(i):
        return remote(g.at[i, other], xb.at[i], sx.at[i], rx.at[i], partner)

    def copy_a(i):
        return remote(sb.at[i], ab.at[i], ss.at[i], ra.at[i], inner)

    def copy_b(i):
        return remote(sb.at[i], bb.at[i], ss.at[i], rb.at[i], across)

    def copy_c(i):
        return remote(tot.at[i, own], tot.at[i, own], sc.at[i], rc.at[i], outer)

    def copy_y(i):
        return remote(tot.at[i, own], tot.at[i, own], sy.at[i], ry.at[i], partner)

    def copy_out(j):
        i = lax.rem(j, LAST)
        s = lax.div(j, 3)
        row = (1 - lax.div(s, SLICES)) * 3 + lax.rem(j, 3)
        cols = pl.ds(pl.multiple_of(lax.rem(s, SLICES) * FS, FS), FS)
        return pltpu.make_async_copy(tot.at[i], out.at[row, :, cols], so.at[i])

    def stage(j, only=None):
        cond = (j >= 0) & (j < CHUNKS)
        if only is not None:
            cond = cond & only
        return pl.when(cond)

    def tick(k):
        @stage(k)
        def _():
            copy_x(lax.rem(k, SLOTS)).start()

        j1 = k - 1

        @stage(j1)
        def _():
            i = lax.rem(j1, SLOTS)
            copy_x(i).wait_recv()
            copy_x(i).wait_send()

            @pl.when(is_end)
            def _():
                sb[i] = (g[i, own].astype(F32) + xb[i].astype(F32)).astype(BF16)
                copy_a(i).start()

        j2 = k - 3

        @stage(j2, is_mid)
        def _():
            i = lax.rem(j2, SLOTS)
            copy_a(i).wait_recv()
            sb[i] = (g[i, own].astype(F32) + xb[i].astype(F32) + ab[i].astype(F32)).astype(BF16)
            copy_b(i).start()

        j3 = k - 5

        @stage(j3, is_mid)
        def _():
            i, t = lax.rem(j3, SLOTS), lax.rem(j3, LAST)
            copy_b(i).wait_recv()
            tot[t, own] = (sb[i].astype(F32) + bb[i].astype(F32)).astype(BF16)
            copy_c(t).start()
            copy_y(t).start()
            copy_b(i).wait_send()

        j4 = k - 7

        @stage(j4, is_end)
        def _():
            i, t = lax.rem(j4, SLOTS), lax.rem(j4, LAST)
            copy_c(t).wait_recv()
            copy_y(t).start()
            copy_a(i).wait_send()

        j5 = k - 8

        @stage(j5)
        def _():
            t = lax.rem(j5, LAST)
            copy_y(t).wait_recv()
            copy_y(t).wait_send()

            @pl.when(is_mid)
            def _():
                copy_c(t).wait_send()

            copy_out(j5).start()

        j6 = k - 9

        @stage(j6)
        def _():
            copy_out(j6).wait()

    def transpose(src, dst):
        for r in range(T // ROWS):
            dst[:, r * ROWS : (r + 1) * ROWS] = src[r * ROWS : (r + 1) * ROWS, :].T

    def slice_(s, _):
        slot = lax.rem(s, 2)
        layer = 1 - lax.div(s, SLICES)

        @pl.when(s == 0)
        def _():
            loads[0].wait()
            loads[1].wait()

        for copy in weights(s):
            copy.wait()

        @pl.when(s + 1 < 2 * SLICES)
        def _():
            for copy in weights(s + 1):
                copy.start()

        @pl.when(s == SLICES)
        def _():
            loads[2].wait()
            loads[3].wait()

            def block(r, _):
                rows = pl.ds(pl.multiple_of(r * ROWS, ROWS), ROWS)
                wide = h[rows].astype(F32)
                by_a = da[rows].astype(BF16).astype(F32)
                scale = lax.rsqrt(jnp.mean(wide * wide, -1, keepdims=True) + 1e-6)
                back = jnp.mean(by_a * wide, -1, keepdims=True) * (scale * scale * scale)
                by_h = (by_a * scale - wide * back).astype(BF16)
                dz[rows] = (dz[rows].astype(F32) + by_h.astype(F32)).astype(BF16)
                return ()

            lax.fori_loop(0, T // ROWS, block, ())

        def block(r, _):
            rows = pl.ds(pl.multiple_of(r * ROWS, ROWS), ROWS)
            both = jnp.dot(a[layer, rows], wgu[slot], preferred_element_type=F32)
            gate, up = both[:, :FS], both[:, FS:]
            by_act = dot_t(dz[rows], wd[slot]).astype(BF16).astype(F32)
            sig = jax.nn.sigmoid(gate)
            silu = gate * sig
            act[rows] = (silu * up).astype(BF16)
            by_gate = (by_act * up * (sig * (1 + gate * (1 - sig)))).astype(BF16)
            by_up = (by_act * silu).astype(BF16)
            dgu[rows, :FS] = by_gate
            dgu[rows, FS:] = by_up

            @pl.when(s < SLICES)
            def _():
                part = dot_t(dgu[rows], wgu[slot])

                @pl.when(s == 0)
                def _():
                    da[rows] = part

                @pl.when(s > 0)
                def _():
                    da[rows] += part

            return ()

        half = T // ROWS // 2
        lax.fori_loop(0, half, block, ())
        tick(3 * s - 1)
        lax.fori_loop(half, 2 * half, block, ())

        @pl.when(lax.rem(s, SLICES) == 0)
        def _():
            transpose(dz, dzt)
            transpose(a.at[layer], at)

        g[lax.rem(3 * s, SLOTS)] = jnp.dot(dzt[...], act[...], preferred_element_type=F32).astype(BF16)
        tick(3 * s)
        both = jnp.dot(at[...], dgu[...], preferred_element_type=F32).astype(BF16)
        g[lax.rem(3 * s + 1, SLOTS)] = both[:, :FS]
        g[lax.rem(3 * s + 2, SLOTS)] = both[:, FS:]
        tick(3 * s + 1)
        return ()

    lax.fori_loop(0, 2 * SLICES, slice_, ())

    def drain(k, _):
        tick(k)
        return ()

    lax.fori_loop(CHUNKS - 1, CHUNKS + 10, drain, ())


def gradients(a0, a1, h1, dy, wg, wu, wd):
    dma = lambda *n: pltpu.SemaphoreType.DMA(n)
    any_ = pl.BlockSpec(memory_space=pl.ANY)
    return pl.pallas_call(
        kernel,
        out_shape=jax.ShapeDtypeStruct((6, D, FF), BF16),
        in_specs=[any_] * 7,
        out_specs=any_,
        scratch_shapes=[
            pltpu.VMEM((2, T, D), BF16),
            pltpu.VMEM((D, T), BF16),
            pltpu.VMEM((T, D), BF16),
            pltpu.VMEM((D, T), BF16),
            pltpu.VMEM((T, D), BF16),
            pltpu.VMEM((T, D), F32),
            pltpu.VMEM((2, D, 2 * FS), BF16),
            pltpu.VMEM((2, FS, D), BF16),
            pltpu.VMEM((T, FS), BF16),
            pltpu.VMEM((T, 2 * FS), BF16),
            pltpu.VMEM((SLOTS, D, FS), BF16),
            pltpu.VMEM((SLOTS, HALF, FS), BF16),
            pltpu.VMEM((SLOTS, HALF, FS), BF16),
            pltpu.VMEM((SLOTS, HALF, FS), BF16),
            pltpu.VMEM((SLOTS, HALF, FS), BF16),
            pltpu.VMEM((LAST, D, FS), BF16),
            dma(4),
            dma(2, 3),
        ]
        + [dma(SLOTS)] * 5
        + [dma(LAST)] * 5,
        compiler_params=pltpu.CompilerParams(collective_id=0, has_side_effects=True, vmem_limit_bytes=60 * 2**20),
        cost_estimate=pl.CostEstimate(flops=90 * 10**9, bytes_accessed=60 * 2**20, transcendentals=0),
        name="backward_sum",
    )(a0, a1, h1, dy, wg, wu, wd)


def solution(mesh):
    def step(x, dy, *arrays):
        weights, m, v = (arrays[i : i + 3] for i in (0, 3, 6))
        wg, wu, wd = weights
        h0 = x[0]
        a0 = normed(h0)
        gate = jnp.dot(a0, wg[0], preferred_element_type=F32)
        up = jnp.dot(a0, wu[0], preferred_element_type=F32)
        h1 = h0 + matmul((jax.nn.silu(gate) * up).astype(BF16), wd[0])
        a1 = normed(h1)
        summed = gradients(a0, a1, h1, dy[0], wg, wu, wd).reshape(2, 3, D, FF)
        grads = [summed[:, 1], summed[:, 2], jnp.swapaxes(summed[:, 0], 1, 2)]
        new = [adamw(w.astype(F32), m, v, g.astype(F32)) for w, m, v, g in zip(weights, m, v, grads, strict=True)]
        return tuple(one[which] for which in range(3) for one in new)

    return jax.shard_map(
        step,
        mesh=mesh,
        in_specs=(P(("rep", "dp"), None, None),) * 2 + (P(None, None, None),) * 9,
        out_specs=(P("rep", None, None),) * 9,
        check_vma=False,
    )
```

```python
import jax
import jax.numpy as jnp
from jax import lax
from jax.experimental import pallas as pl
from jax.experimental.pallas import tpu as pltpu
from jax.sharding import PartitionSpec as P

T, D, FF = 2048, 640, 2048
FS = 256
SLICES = FF // FS
CHUNKS = 2 * SLICES * 3
PARTS = 2
UNITS = CHUNKS * PARTS
SLOTS = 8
MESSAGES = SLOTS * PARTS
LAST = 12
HALF = D // 2
PIECE = HALF // PARTS
ROWS = 512
FROWS = 512
NROWS = 256
F32, BF16 = jnp.float32, jnp.bfloat16
MESH = pl.DeviceIdType.MESH


def normed(h):
    wide = h.astype(F32)
    scale = lax.rsqrt(jnp.mean(wide**2, -1, keepdims=True) + 1e-6)
    return (wide * scale).astype(BF16)


def adamw(w, m, v, g):
    m = 0.9 * m + 0.1 * g
    v = 0.95 * v + 0.05 * g * g
    step = m * lax.rsqrt(v + 1e-8) + 0.1 * w
    return (w - 0.02 * step).astype(BF16), m, v


AFTER = (2, 5, 8, 11, 13, 14)


def dot_t(a, b):
    return lax.dot_general(a, b, (((1,), (1,)), ((), ())), preferred_element_type=F32)


def kernel(
    x_in, dy_in, wg_in, wu_in, wd_in, out,
    a, at, dz, dzt, h, da, wgu, wd, act, dgu,
    g, xb, ab, bb, sb, tot,
    load_sem, w_sem, sx, rx, ss, ra, rb, sc, rc, sy, ry, so,
):
    at_dp = lax.axis_index("dp")
    c = lax.rem(at_dp, 2)
    z = lax.div(at_dp, 2)
    is_end = (z == 0) | (z == 3)
    is_mid = (z == 1) | (z == 2)
    partner = z * 2 + 1 - c
    inner = jnp.where(z == 0, 1, 2) * 2 + c
    outer = jnp.where(z == 1, 0, 3) * 2 + c
    across = (3 - z) * 2 + c
    def piece(u, core):
        return pl.ds(pl.multiple_of(core * HALF + lax.rem(u, PARTS) * PIECE, PIECE), PIECE)

    def load(src, dst, i):
        return pltpu.make_async_copy(src, dst, load_sem.at[i])

    loads = [load(x_in, h, 0), load(dy_in, dz, 1)]

    def weights(s):
        slot = lax.rem(s + SLICES, 2)
        layer = jnp.where((s >= 0) & (s < SLICES), 1, 0)
        cols = pl.ds(pl.multiple_of(lax.rem(s + SLICES, SLICES) * FS, FS), FS)
        return [
            pltpu.make_async_copy(wg_in.at[layer, :, cols], wgu.at[slot, :, pl.ds(0, FS)], w_sem.at[slot, 0]),
            pltpu.make_async_copy(wu_in.at[layer, :, cols], wgu.at[slot, :, pl.ds(FS, FS)], w_sem.at[slot, 1]),
            pltpu.make_async_copy(wd_in.at[layer, cols, :], wd.at[slot], w_sem.at[slot, 2]),
        ]

    loads[0].start()
    for copy in weights(-SLICES):
        copy.start()
    loads[1].start()

    barrier = pltpu.get_barrier_semaphore()

    def greet(device):
        pl.semaphore_signal(barrier, inc=1, device_id={"dp": device}, device_id_type=MESH)

    greet(partner)

    @pl.when(is_end)
    def _():
        greet(inner)
        pl.semaphore_wait(barrier, 2)

    @pl.when(is_mid)
    def _():
        greet(outer)
        greet(across)
        pl.semaphore_wait(barrier, 3)

    def remote(src, dst, send, recv, device):
        return pltpu.make_async_remote_copy(
            src_ref=src, dst_ref=dst, send_sem=send, recv_sem=recv, device_id={"dp": device}, device_id_type=MESH
        )

    def chunk(u):
        return lax.rem(lax.div(u, PARTS), SLOTS)

    def sums(u):
        return tot.at[lax.rem(lax.div(u, PARTS), LAST), piece(u, c)]

    def copy_x(u):
        i = lax.rem(u, MESSAGES)
        return remote(g.at[chunk(u), piece(u, 1 - c)], xb.at[i], sx.at[i], rx.at[i], partner)

    def copy_a(u):
        i = lax.rem(u, MESSAGES)
        return remote(sb.at[i], ab.at[i], ss.at[i], ra.at[i], inner)

    def copy_b(u):
        i = lax.rem(u, MESSAGES)
        return remote(sb.at[i], bb.at[i], ss.at[i], rb.at[i], across)

    def copy_c(u):
        i = lax.rem(u, LAST * PARTS)
        return remote(sums(u), sums(u), sc.at[i], rc.at[i], outer)

    def copy_y(u):
        i = lax.rem(u, LAST * PARTS)
        return remote(sums(u), sums(u), sy.at[i], ry.at[i], partner)

    def copy_out(u):
        k = lax.div(u, PARTS)
        i = lax.rem(k, LAST)
        s = lax.div(k, 3)
        row = (1 - lax.div(s, SLICES)) * 3 + lax.rem(k, 3)
        cols = pl.ds(pl.multiple_of(lax.rem(s, SLICES) * FS, FS), FS)
        return pltpu.make_async_copy(tot.at[i], out.at[row, :, cols], so.at[i])

    def stage(u, only=None):
        cond = (u >= 0) & (u < UNITS)
        if only is not None:
            cond = cond & only
        return pl.when(cond)

    def tick(u):
        @stage(u)
        def _():
            copy_x(u).start()

        u1 = u - AFTER[0]

        @stage(u1)
        def _():
            i = lax.rem(u1, MESSAGES)
            copy_x(u1).wait_recv()
            copy_x(u1).wait_send()

            @pl.when(is_end)
            def _():
                sb[i] = (g[chunk(u1), piece(u1, c)].astype(F32) + xb[i].astype(F32)).astype(BF16)
                copy_a(u1).start()

        u2 = u - AFTER[1]

        @stage(u2, is_mid)
        def _():
            i = lax.rem(u2, MESSAGES)
            copy_a(u2).wait_recv()
            sb[i] = (g[chunk(u2), piece(u2, c)].astype(F32) + xb[i].astype(F32) + ab[i].astype(F32)).astype(BF16)
            copy_b(u2).start()

        u3 = u - AFTER[2]

        @stage(u3, is_mid)
        def _():
            i = lax.rem(u3, MESSAGES)
            copy_b(u3).wait_recv()
            tot[lax.rem(lax.div(u3, PARTS), LAST), piece(u3, c)] = (sb[i].astype(F32) + bb[i].astype(F32)).astype(BF16)
            copy_c(u3).start()
            copy_y(u3).start()
            copy_b(u3).wait_send()

        u4 = u - AFTER[3]

        @stage(u4, is_end)
        def _():
            copy_c(u4).wait_recv()
            copy_y(u4).start()
            copy_a(u4).wait_send()

        u5 = u - AFTER[4]

        @stage(u5)
        def _():
            copy_y(u5).wait_recv()
            copy_y(u5).wait_send()

            @pl.when(is_mid)
            def _():
                copy_c(u5).wait_send()

            @pl.when(lax.rem(u5, PARTS) == PARTS - 1)
            def _():
                copy_out(u5).start()

        u6 = u - AFTER[5]

        @stage(u6, lax.rem(u6, PARTS) == PARTS - 1)
        def _():
            copy_out(u6).wait()

    def take_weights(s):
        for copy in weights(s):
            copy.wait()

        @pl.when(s + 1 < 2 * SLICES)
        def _():
            for copy in weights(s + 1):
                copy.start()

    def block_rows(r):
        return pl.ds(pl.multiple_of(r * ROWS, ROWS), ROWS)

    def norm_rows(r):
        return pl.ds(pl.multiple_of(r * NROWS, NROWS), NROWS)

    def each_norm(body):
        lax.fori_loop(0, T // NROWS, body, ())

    def each_block(body):
        lax.fori_loop(0, T // ROWS, body, ())

    loads[0].wait()

    def first_norm(r, _):
        rows = norm_rows(r)
        inputs = normed(h[rows])
        a[0, rows] = inputs
        at[0, :, rows] = inputs.T
        da[rows] = jnp.zeros((NROWS, D), F32)
        return ()

    each_norm(first_norm)
    loads[1].wait()

    def forward(f, _):
        slot = lax.rem(f, 2)
        take_weights(f - SLICES)
        turn = pl.ds(pl.multiple_of(f * FS, FS), FS)
        dzt[:, turn] = dz[turn].T
        for r in range(T // FROWS):
            rows = pl.ds(r * FROWS, FROWS)
            both = jnp.dot(a[0, rows], wgu[slot], preferred_element_type=F32)
            gate, up = both[:, :FS], both[:, FS:]
            hidden = (gate * jax.nn.sigmoid(gate) * up).astype(BF16)
            da[rows] += jnp.dot(hidden, wd[slot], preferred_element_type=F32)
        return ()

    lax.fori_loop(0, SLICES, forward, ())

    def second_norm(r, _):
        rows = norm_rows(r)
        states = (h[rows].astype(F32) + da[rows].astype(BF16).astype(F32)).astype(BF16)
        h[rows] = states
        inputs = normed(states)
        a[1, rows] = inputs
        at[1, :, rows] = inputs.T
        da[rows] = jnp.zeros((NROWS, D), F32)
        return ()

    each_norm(second_norm)

    def backward(s, layer):
        slot = lax.rem(s, 2)
        take_weights(s)

        def block(r, _):
            rows = block_rows(r)
            both = jnp.dot(a[layer, rows], wgu[slot], preferred_element_type=F32)
            gate, up = both[:, :FS], both[:, FS:]
            by_act = dot_t(dz[rows], wd[slot]).astype(BF16).astype(F32)
            sig = jax.nn.sigmoid(gate)
            silu = gate * sig
            act[rows] = (silu * up).astype(BF16)
            dgu[rows, :FS] = (by_act * up * (sig * (1 + gate * (1 - sig)))).astype(BF16)
            dgu[rows, FS:] = (by_act * silu).astype(BF16)
            if layer == 1:
                da[rows] += dot_t(dgu[rows], wgu[slot])
            tick(6 * s - 4 + r)
            return ()

        each_block(block)
        g[lax.rem(3 * s, SLOTS)] = jnp.dot(dzt[...], act[...], preferred_element_type=F32).astype(BF16)
        tick(6 * s)
        both = jnp.dot(at[layer], dgu[...], preferred_element_type=F32).astype(BF16)
        g[lax.rem(3 * s + 1, SLOTS)] = both[:, :FS]
        g[lax.rem(3 * s + 2, SLOTS)] = both[:, FS:]
        tick(6 * s + 1)

    def last_layer(s, _):
        backward(s, 1)
        return ()

    def first_layer(s, _):
        backward(s, 0)
        return ()

    lax.fori_loop(0, SLICES, last_layer, ())

    def between(r, _):
        rows = norm_rows(r)
        wide = h[rows].astype(F32)
        by_a = da[rows].astype(BF16).astype(F32)
        scale = lax.rsqrt(jnp.mean(wide * wide, -1, keepdims=True) + 1e-6)
        back = jnp.mean(by_a * wide, -1, keepdims=True) * (scale * scale * scale)
        by_h = (by_a * scale - wide * back).astype(BF16)
        total = (dz[rows].astype(F32) + by_h.astype(F32)).astype(BF16)
        dz[rows] = total
        dzt[:, rows] = total.T
        return ()

    each_norm(between)
    lax.fori_loop(SLICES, 2 * SLICES, first_layer, ())

    def drain(u, _):
        tick(u)
        return ()

    lax.fori_loop(UNITS - 4, UNITS + AFTER[-1] + 1, drain, ())


def gradients(x, dy, wg, wu, wd):
    dma = lambda *n: pltpu.SemaphoreType.DMA(n)
    any_ = pl.BlockSpec(memory_space=pl.ANY)
    return pl.pallas_call(
        kernel,
        out_shape=jax.ShapeDtypeStruct((6, D, FF), BF16),
        in_specs=[any_] * 5,
        out_specs=any_,
        scratch_shapes=[
            pltpu.VMEM((2, T, D), BF16),
            pltpu.VMEM((2, D, T), BF16),
            pltpu.VMEM((T, D), BF16),
            pltpu.VMEM((D, T), BF16),
            pltpu.VMEM((T, D), BF16),
            pltpu.VMEM((T, D), F32),
            pltpu.VMEM((2, D, 2 * FS), BF16),
            pltpu.VMEM((2, FS, D), BF16),
            pltpu.VMEM((T, FS), BF16),
            pltpu.VMEM((T, 2 * FS), BF16),
            pltpu.VMEM((SLOTS, D, FS), BF16),
            pltpu.VMEM((MESSAGES, PIECE, FS), BF16),
            pltpu.VMEM((MESSAGES, PIECE, FS), BF16),
            pltpu.VMEM((MESSAGES, PIECE, FS), BF16),
            pltpu.VMEM((MESSAGES, PIECE, FS), BF16),
            pltpu.VMEM((LAST, D, FS), BF16),
            dma(2),
            dma(2, 3),
        ]
        + [dma(MESSAGES)] * 5
        + [dma(LAST * PARTS)] * 4
        + [dma(LAST)],
        compiler_params=pltpu.CompilerParams(collective_id=0, has_side_effects=True, vmem_limit_bytes=63 * 2**20),
        cost_estimate=pl.CostEstimate(flops=95 * 10**9, bytes_accessed=60 * 2**20, transcendentals=0),
        name="backward_sum",
    )(x, dy, wg, wu, wd)


def adamw_kernel(*refs):
    g_refs, w_refs, m_refs, v_refs, wo_refs, mo_refs, vo_refs = (refs[i : i + 3] for i in range(0, 21, 3))
    turned = refs[21]
    turned[...] = g_refs[2][0].T
    for n in range(3):
        count, rows = (5, 16) if n < 2 else (8, 32)

        def part(r, _, n=n, rows=rows):
            at = pl.ds(pl.multiple_of(r * rows, rows), rows)
            g = (g_refs[n][0, at] if n < 2 else turned[at]).astype(F32)
            w, m, v = adamw(w_refs[n][0, at].astype(F32), m_refs[n][0, at], v_refs[n][0, at], g)
            wo_refs[n][0, at] = w
            mo_refs[n][0, at] = m
            vo_refs[n][0, at] = v
            return ()

        lax.fori_loop(0, count, part, (), unroll=True)


def optimizer(summed, weights, m, v):
    steps = 8
    wide = pl.BlockSpec((1, D // steps, FF), lambda l, i: (l, i, 0))
    tall = pl.BlockSpec((1, FF // steps, D), lambda l, i: (l, i, 0))
    each = [wide, wide, tall]
    g_specs = [
        pl.BlockSpec((1, D // steps, FF), lambda l, i: (3 * l + 1, i, 0)),
        pl.BlockSpec((1, D // steps, FF), lambda l, i: (3 * l + 2, i, 0)),
        pl.BlockSpec((1, D, FF // steps), lambda l, i: (3 * l, 0, i)),
    ]
    shapes = [jax.ShapeDtypeStruct(one.shape, one.dtype) for one in (*weights, *m, *v)]
    return pl.pallas_call(
        adamw_kernel,
        grid=(2, steps),
        out_shape=shapes,
        in_specs=g_specs + each * 3,
        out_specs=each * 3,
        scratch_shapes=[pltpu.VMEM((FF // steps, D), BF16)],
        compiler_params=pltpu.CompilerParams(vmem_limit_bytes=63 * 2**20),
        cost_estimate=pl.CostEstimate(flops=120 * 10**6, bytes_accessed=173 * 10**6, transcendentals=8 * 10**6),
        name="adamw",
    )(summed, summed, summed, *weights, *m, *v)


def solution(mesh):
    def step(x, dy, *arrays):
        weights, m, v = (arrays[i : i + 3] for i in (0, 3, 6))
        summed = gradients(x[0], dy[0], *weights)
        return tuple(optimizer(summed, weights, m, v))

    return jax.shard_map(
        step,
        mesh=mesh,
        in_specs=(P(("rep", "dp"), None, None),) * 2 + (P(None, None, None),) * 9,
        out_specs=(P("rep", None, None),) * 9,
        check_vma=False,
    )
```

```python
import jax
import jax.numpy as jnp
from jax import lax
from jax.experimental import pallas as pl
from jax.experimental.pallas import tpu as pltpu
from jax.sharding import PartitionSpec as P

T, D, FF = 2048, 640, 2048
FS = 256
SLICES = FF // FS
CHUNKS = 2 * SLICES * 3
PARTS = 2
UNITS = CHUNKS * PARTS
SLOTS = 8
MESSAGES = SLOTS * PARTS
LAST = 12
HALF = D // 2
PIECE = HALF // PARTS
ROWS = 512
FROWS = 2048
NROWS = 256
F32, BF16 = jnp.float32, jnp.bfloat16
MESH = pl.DeviceIdType.MESH


def normed(h):
    wide = h.astype(F32)
    scale = lax.rsqrt(jnp.mean(wide**2, -1, keepdims=True) + 1e-6)
    return (wide * scale).astype(BF16)


def adamw(w, m, v, g):
    m = 0.9 * m + 0.1 * g
    v = 0.95 * v + 0.05 * g * g
    step = m * lax.rsqrt(v + 1e-8) + 0.1 * w
    return (w - 0.02 * step).astype(BF16), m, v


AFTER = (1, 4, 7, 10, 12, 13)


def dot_t(a, b):
    return lax.dot_general(a, b, (((1,), (1,)), ((), ())), preferred_element_type=F32)


def kernel(
    x_in, dy_in, wg_in, wu_in, wd_in, out,
    a, at, dz, dzt, h, da, wgu, wd, act, dgu,
    g, xb, ab, bb, sb, tot,
    load_sem, w_sem, sx, rx, ss, ra, rb, sc, rc, sy, ry, so,
):
    at_dp = lax.axis_index("dp")
    c = lax.rem(at_dp, 2)
    z = lax.div(at_dp, 2)
    is_end = (z == 0) | (z == 3)
    is_mid = (z == 1) | (z == 2)
    partner = z * 2 + 1 - c
    inner = jnp.where(z == 0, 1, 2) * 2 + c
    outer = jnp.where(z == 1, 0, 3) * 2 + c
    across = (3 - z) * 2 + c
    def piece(u, core):
        return pl.ds(pl.multiple_of(core * HALF + lax.rem(u, PARTS) * PIECE, PIECE), PIECE)

    def load(src, dst, i):
        return pltpu.make_async_copy(src, dst, load_sem.at[i])

    loads = [load(x_in, h, 0), load(dy_in, dz, 1)]

    def weights(s):
        slot = lax.rem(s + SLICES, 2)
        layer = jnp.where((s >= 0) & (s < SLICES), 1, 0)
        cols = pl.ds(pl.multiple_of(lax.rem(s + SLICES, SLICES) * FS, FS), FS)
        return [
            pltpu.make_async_copy(wg_in.at[layer, :, cols], wgu.at[slot, :, pl.ds(0, FS)], w_sem.at[slot, 0]),
            pltpu.make_async_copy(wu_in.at[layer, :, cols], wgu.at[slot, :, pl.ds(FS, FS)], w_sem.at[slot, 1]),
            pltpu.make_async_copy(wd_in.at[layer, cols, :], wd.at[slot], w_sem.at[slot, 2]),
        ]

    loads[0].start()
    for copy in weights(-SLICES):
        copy.start()
    loads[1].start()

    barrier = pltpu.get_barrier_semaphore()

    def greet(device):
        pl.semaphore_signal(barrier, inc=1, device_id={"dp": device}, device_id_type=MESH)

    greet(partner)

    @pl.when(is_end)
    def _():
        greet(inner)
        pl.semaphore_wait(barrier, 2)

    @pl.when(is_mid)
    def _():
        greet(outer)
        greet(across)
        pl.semaphore_wait(barrier, 3)

    def remote(src, dst, send, recv, device):
        return pltpu.make_async_remote_copy(
            src_ref=src, dst_ref=dst, send_sem=send, recv_sem=recv, device_id={"dp": device}, device_id_type=MESH
        )

    def chunk(u):
        return lax.rem(lax.div(u, PARTS), SLOTS)

    def sums(u):
        return tot.at[lax.rem(lax.div(u, PARTS), LAST), piece(u, c)]

    def copy_x(u):
        i = lax.rem(u, MESSAGES)
        return remote(g.at[chunk(u), piece(u, 1 - c)], xb.at[i], sx.at[i], rx.at[i], partner)

    def copy_a(u):
        i = lax.rem(u, MESSAGES)
        return remote(sb.at[i], ab.at[i], ss.at[i], ra.at[i], inner)

    def copy_b(u):
        i = lax.rem(u, MESSAGES)
        return remote(sb.at[i], bb.at[i], ss.at[i], rb.at[i], across)

    def copy_c(u):
        i = lax.rem(u, LAST * PARTS)
        return remote(sums(u), sums(u), sc.at[i], rc.at[i], outer)

    def copy_y(u):
        i = lax.rem(u, LAST * PARTS)
        return remote(sums(u), sums(u), sy.at[i], ry.at[i], partner)

    def copy_out(u):
        k = lax.div(u, PARTS)
        i = lax.rem(k, LAST)
        s = lax.div(k, 3)
        row = (1 - lax.div(s, SLICES)) * 3 + lax.rem(k, 3)
        cols = pl.ds(pl.multiple_of(lax.rem(s, SLICES) * FS, FS), FS)
        return pltpu.make_async_copy(tot.at[i], out.at[row, :, cols], so.at[i])

    def stage(u, only=None):
        cond = (u >= 0) & (u < UNITS)
        if only is not None:
            cond = cond & only
        return pl.when(cond)

    def tick(u):
        @stage(u)
        def _():
            copy_x(u).start()

        u1 = u - AFTER[0]

        @stage(u1)
        def _():
            i = lax.rem(u1, MESSAGES)
            copy_x(u1).wait_recv()
            copy_x(u1).wait_send()

            @pl.when(is_end)
            def _():
                sb[i] = (g[chunk(u1), piece(u1, c)].astype(F32) + xb[i].astype(F32)).astype(BF16)
                copy_a(u1).start()

        u2 = u - AFTER[1]

        @stage(u2, is_mid)
        def _():
            i = lax.rem(u2, MESSAGES)
            copy_a(u2).wait_recv()
            sb[i] = (g[chunk(u2), piece(u2, c)].astype(F32) + xb[i].astype(F32) + ab[i].astype(F32)).astype(BF16)
            copy_b(u2).start()

        u3 = u - AFTER[2]

        @stage(u3, is_mid)
        def _():
            i = lax.rem(u3, MESSAGES)
            copy_b(u3).wait_recv()
            tot[lax.rem(lax.div(u3, PARTS), LAST), piece(u3, c)] = (sb[i].astype(F32) + bb[i].astype(F32)).astype(BF16)
            copy_c(u3).start()
            copy_y(u3).start()
            copy_b(u3).wait_send()

        u4 = u - AFTER[3]

        @stage(u4, is_end)
        def _():
            copy_c(u4).wait_recv()
            copy_y(u4).start()
            copy_a(u4).wait_send()

        u5 = u - AFTER[4]

        @stage(u5)
        def _():
            copy_y(u5).wait_recv()
            copy_y(u5).wait_send()

            @pl.when(is_mid)
            def _():
                copy_c(u5).wait_send()

            @pl.when(lax.rem(u5, PARTS) == PARTS - 1)
            def _():
                copy_out(u5).start()

        u6 = u - AFTER[5]

        @stage(u6, lax.rem(u6, PARTS) == PARTS - 1)
        def _():
            copy_out(u6).wait()

    def take_weights(s):
        for copy in weights(s):
            copy.wait()

        @pl.when(s + 1 < 2 * SLICES)
        def _():
            for copy in weights(s + 1):
                copy.start()

    def block_rows(r):
        return pl.ds(pl.multiple_of(r * ROWS, ROWS), ROWS)

    def norm_rows(r):
        return pl.ds(pl.multiple_of(r * NROWS, NROWS), NROWS)

    def each_norm(body):
        lax.fori_loop(0, T // NROWS, body, ())

    def each_block(body):
        lax.fori_loop(0, T // ROWS, body, ())

    loads[0].wait()

    def first_norm(r, _):
        rows = norm_rows(r)
        inputs = normed(h[rows])
        a[0, rows] = inputs
        at[0, :, rows] = inputs.T
        da[rows] = jnp.zeros((NROWS, D), F32)
        return ()

    each_norm(first_norm)
    loads[1].wait()

    def forward(f, _):
        slot = lax.rem(f, 2)
        take_weights(f - SLICES)
        turn = pl.ds(pl.multiple_of(f * FS, FS), FS)
        dzt[:, turn] = dz[turn].T
        for r in range(T // FROWS):
            rows = pl.ds(r * FROWS, FROWS)
            both = jnp.dot(a[0, rows], wgu[slot], preferred_element_type=F32)
            gate, up = both[:, :FS], both[:, FS:]
            hidden = (gate * jax.nn.sigmoid(gate) * up).astype(BF16)
            da[rows] += jnp.dot(hidden, wd[slot], preferred_element_type=F32)
        return ()

    lax.fori_loop(0, SLICES, forward, ())

    def second_norm(r, _):
        rows = norm_rows(r)
        states = (h[rows].astype(F32) + da[rows].astype(BF16).astype(F32)).astype(BF16)
        h[rows] = states
        inputs = normed(states)
        a[1, rows] = inputs
        at[1, :, rows] = inputs.T
        da[rows] = jnp.zeros((NROWS, D), F32)
        return ()

    each_norm(second_norm)

    def backward(s, layer):
        slot = lax.rem(s, 2)
        take_weights(s)

        def block(r, _):
            rows = block_rows(r)
            both = jnp.dot(a[layer, rows], wgu[slot], preferred_element_type=F32)
            gate, up = both[:, :FS], both[:, FS:]
            by_act = dot_t(dz[rows], wd[slot]).astype(BF16).astype(F32)
            sig = jax.nn.sigmoid(gate)
            silu = gate * sig
            act[rows] = (silu * up).astype(BF16)
            dgu[rows, :FS] = (by_act * up * (sig * (1 + gate * (1 - sig)))).astype(BF16)
            dgu[rows, FS:] = (by_act * silu).astype(BF16)
            if layer == 1:
                da[rows] += dot_t(dgu[rows], wgu[slot])
            tick(6 * s - 4 + r)
            return ()

        each_block(block)
        g[lax.rem(3 * s, SLOTS)] = jnp.dot(dzt[...], act[...], preferred_element_type=F32).astype(BF16)
        tick(6 * s)
        both = jnp.dot(at[layer], dgu[...], preferred_element_type=F32).astype(BF16)
        g[lax.rem(3 * s + 1, SLOTS)] = both[:, :FS]
        g[lax.rem(3 * s + 2, SLOTS)] = both[:, FS:]
        tick(6 * s + 1)

    def last_layer(s, _):
        backward(s, 1)
        return ()

    def first_layer(s, _):
        backward(s, 0)
        return ()

    lax.fori_loop(0, SLICES, last_layer, ())

    def between(r, _):
        rows = norm_rows(r)
        wide = h[rows].astype(F32)
        by_a = da[rows].astype(BF16).astype(F32)
        scale = lax.rsqrt(jnp.mean(wide * wide, -1, keepdims=True) + 1e-6)
        back = jnp.mean(by_a * wide, -1, keepdims=True) * (scale * scale * scale)
        by_h = (by_a * scale - wide * back).astype(BF16)
        total = (dz[rows].astype(F32) + by_h.astype(F32)).astype(BF16)
        dz[rows] = total
        dzt[:, rows] = total.T
        return ()

    each_norm(between)
    lax.fori_loop(SLICES, 2 * SLICES, first_layer, ())

    def drain(u, _):
        tick(u)
        return ()

    lax.fori_loop(UNITS - 4, UNITS + AFTER[-1] + 1, drain, ())


def gradients(x, dy, wg, wu, wd):
    dma = lambda *n: pltpu.SemaphoreType.DMA(n)
    any_ = pl.BlockSpec(memory_space=pl.ANY)
    return pl.pallas_call(
        kernel,
        out_shape=jax.ShapeDtypeStruct((6, D, FF), BF16),
        in_specs=[any_] * 5,
        out_specs=any_,
        scratch_shapes=[
            pltpu.VMEM((2, T, D), BF16),
            pltpu.VMEM((2, D, T), BF16),
            pltpu.VMEM((T, D), BF16),
            pltpu.VMEM((D, T), BF16),
            pltpu.VMEM((T, D), BF16),
            pltpu.VMEM((T, D), F32),
            pltpu.VMEM((2, D, 2 * FS), BF16),
            pltpu.VMEM((2, FS, D), BF16),
            pltpu.VMEM((T, FS), BF16),
            pltpu.VMEM((T, 2 * FS), BF16),
            pltpu.VMEM((SLOTS, D, FS), BF16),
            pltpu.VMEM((MESSAGES, PIECE, FS), BF16),
            pltpu.VMEM((MESSAGES, PIECE, FS), BF16),
            pltpu.VMEM((MESSAGES, PIECE, FS), BF16),
            pltpu.VMEM((MESSAGES, PIECE, FS), BF16),
            pltpu.VMEM((LAST, D, FS), BF16),
            dma(2),
            dma(2, 3),
        ]
        + [dma(MESSAGES)] * 5
        + [dma(LAST * PARTS)] * 4
        + [dma(LAST)],
        compiler_params=pltpu.CompilerParams(collective_id=0, has_side_effects=True, vmem_limit_bytes=63 * 2**20),
        cost_estimate=pl.CostEstimate(flops=95 * 10**9, bytes_accessed=60 * 2**20, transcendentals=0),
        name="backward_sum",
    )(x, dy, wg, wu, wd)


def adamw_kernel(*refs):
    g_refs, w_refs, m_refs, v_refs, wo_refs, mo_refs, vo_refs = (refs[i : i + 3] for i in range(0, 21, 3))
    turned = refs[21]
    turned[...] = g_refs[2][0].T
    for n in range(3):
        count, rows = (5, 16) if n < 2 else (8, 32)

        def part(r, _, n=n, rows=rows):
            at = pl.ds(pl.multiple_of(r * rows, rows), rows)
            g = (g_refs[n][0, at] if n < 2 else turned[at]).astype(F32)
            w, m, v = adamw(w_refs[n][0, at].astype(F32), m_refs[n][0, at], v_refs[n][0, at], g)
            wo_refs[n][0, at] = w
            mo_refs[n][0, at] = m
            vo_refs[n][0, at] = v
            return ()

        lax.fori_loop(0, count, part, (), unroll=True)


def optimizer(summed, weights, m, v):
    steps = 8
    wide = pl.BlockSpec((1, D // steps, FF), lambda l, i: (l, i, 0))
    tall = pl.BlockSpec((1, FF // steps, D), lambda l, i: (l, i, 0))
    each = [wide, wide, tall]
    g_specs = [
        pl.BlockSpec((1, D // steps, FF), lambda l, i: (3 * l + 1, i, 0)),
        pl.BlockSpec((1, D // steps, FF), lambda l, i: (3 * l + 2, i, 0)),
        pl.BlockSpec((1, D, FF // steps), lambda l, i: (3 * l, 0, i)),
    ]
    shapes = [jax.ShapeDtypeStruct(one.shape, one.dtype) for one in (*weights, *m, *v)]
    return pl.pallas_call(
        adamw_kernel,
        grid=(2, steps),
        out_shape=shapes,
        in_specs=g_specs + each * 3,
        out_specs=each * 3,
        scratch_shapes=[pltpu.VMEM((FF // steps, D), BF16)],
        compiler_params=pltpu.CompilerParams(vmem_limit_bytes=63 * 2**20),
        cost_estimate=pl.CostEstimate(flops=120 * 10**6, bytes_accessed=173 * 10**6, transcendentals=8 * 10**6),
        name="adamw",
    )(summed, summed, summed, *weights, *m, *v)


def solution(mesh):
    def step(x, dy, *arrays):
        weights, m, v = (arrays[i : i + 3] for i in (0, 3, 6))
        summed = gradients(x[0], dy[0], *weights)
        return tuple(optimizer(summed, weights, m, v))

    return jax.shard_map(
        step,
        mesh=mesh,
        in_specs=(P(("rep", "dp"), None, None),) * 2 + (P(None, None, None),) * 9,
        out_specs=(P("rep", None, None),) * 9,
        check_vma=False,
    )
```
